32 devices in a mesh: rep: 2 (over z, core), dp: 16 (over x, y).
Axes of the slice: x: 4, y: 4, z: 1, core: 2. Of those that a mesh axis runs over, the one named last changes fastest.
The devices are a block of a 4x4x8 slice.
Arguments:
- x: bfloat16 [32, 2048, 768], P(('rep', 'dp')), parts along dimension 0
- dy: bfloat16 [32, 2048, 768], P(('rep', 'dp')), parts along dimension 0
- w_gate: bfloat16 [2, 768, 1792], replicated
- w_up: bfloat16 [2, 768, 1792], replicated
- w_down: bfloat16 [2, 1792, 768], replicated
- m_w_gate: float32 [2, 768, 1792], P(None, 'dp')
- m_w_up: float32 [2, 768, 1792], P(None, 'dp')
- m_w_down: float32 [2, 1792, 768], P(None, 'dp')
- v_w_gate: float32 [2, 768, 1792], P(None, 'dp')
- v_w_up: float32 [2, 768, 1792], P(None, 'dp')
- v_w_down: float32 [2, 1792, 768], P(None, 'dp')
Outputs:
- output 1: bfloat16 [4, 768, 1792], P('rep'), parts along dimension 0
- output 2: bfloat16 [4, 768, 1792], P('rep'), parts along dimension 0
- output 3: bfloat16 [4, 1792, 768], P('rep'), parts along dimension 0
- output 4: float32 [4, 768, 1792], P('rep', 'dp'), parts along dimension 0
- output 5: float32 [4, 768, 1792], P('rep', 'dp'), parts along dimension 0
- output 6: float32 [4, 1792, 768], P('rep', 'dp'), parts along dimension 0
- output 7: float32 [4, 768, 1792], P('rep', 'dp'), parts along dimension 0
- output 8: float32 [4, 768, 1792], P('rep', 'dp'), parts along dimension 0
- output 9: float32 [4, 1792, 768], P('rep', 'dp'), parts along dimension 0
There are 2 independent parts. The reference program is written for one: setup_inputs(seed, part) draws one part's arguments, and reference() takes and returns one part's arrays. A program takes and returns all parts, laid end to end along the dimension named above; an argument that names none is the same for every part.
All inputs are finite; a program needn't handle non-finite values.
Results may differ from the reference program's by a relative error of at most 0.022.
Values are sent between devices in bfloat16 or wider.
A program may use at most 768 MiB of HBM per device.

```python
import jax
import jax.numpy as jnp
from jax import lax

SEQUENCES = 16
TOKENS = 2048
D = 768
FF = 1792
LAYERS = 2
NAMES = ("w_gate", "w_up", "w_down")
SHAPES = {"w_gate": (LAYERS, D, FF), "w_up": (LAYERS, D, FF), "w_down": (LAYERS, FF, D)}


def bump(key, n, height):
    away = (jnp.arange(n, dtype=jnp.int32) - jax.random.randint(key, (), 0, n, jnp.int32)) % n
    return jnp.where(away < n // 8, height, 1.0)


def together(key, own, strength):
    shared = jax.random.normal(key, own.shape[1:], jnp.float32)
    return (own + strength * shared) * lax.rsqrt(1 + strength * strength)


def setup_inputs(seed: int = 0, part: int = 0) -> dict:
    kx, kdy, ka, kb, kz, kf, kh, kl, *keys = jax.random.split(jax.random.key(seed), 8 + 3 * len(NAMES))
    kx, kdy, ka, kb = (jax.random.fold_in(k, part) for k in (kx, kdy, ka, kb))
    kw, km, kv = (keys[i::3] for i in range(3))
    shape = (SEQUENCES, TOKENS, D)
    much_x, much_dy = jax.random.uniform(kz, (2,), jnp.float32, 0.0, 1.0)
    loud = 2.0 ** jax.random.uniform(jax.random.fold_in(kz, 1), (), jnp.float32, -1.0, 2.0)
    layers = 2.0 ** jax.random.uniform(kl, (LAYERS, 1, 1), jnp.float32, -1.0, 1.0)
    x = together(ka, jax.random.normal(kx, shape, jnp.float32), much_x) * bump(kf, D, 4.0)
    dy = together(kb, jax.random.normal(kdy, shape, jnp.float32), much_dy)
    drawn = {"x": x.astype(jnp.bfloat16), "dy": (loud * dy * (SEQUENCES * TOKENS) ** -0.5).astype(jnp.bfloat16)}
    for key, name in zip(kw, NAMES, strict=True):
        w = jax.random.normal(key, SHAPES[name], jnp.float32) * SHAPES[name][1] ** -0.5
        drawn[name] = (w * {"w_gate": 1.0, "w_up": bump(kh, FF, 4.0), "w_down": layers}[name]).astype(jnp.bfloat16)
    for key, name in zip(km, NAMES, strict=True):
        drawn[f"m_{name}"] = 0.1 * jax.random.normal(key, SHAPES[name], jnp.float32)
    for key, name in zip(kv, NAMES, strict=True):
        drawn[f"v_{name}"] = jax.random.uniform(key, SHAPES[name], jnp.float32, 0.005, 0.015)
    return drawn


def matmul(a, w):
    return jnp.dot(a, w, preferred_element_type=jnp.float32).astype(jnp.bfloat16)


def normed(h):
    wide = h.astype(jnp.float32)
    scale = lax.rsqrt(jnp.mean(wide**2, -1, keepdims=True) + 1e-6)
    return (wide * scale).astype(jnp.bfloat16)


def layer(h, w):
    a = normed(h)
    gate = jnp.dot(a, w["w_gate"], preferred_element_type=jnp.float32)
    up = jnp.dot(a, w["w_up"], preferred_element_type=jnp.float32)
    return h + matmul((jax.nn.silu(gate) * up).astype(jnp.bfloat16), w["w_down"])


def adamw(w, m, v, g):
    m = 0.9 * m + 0.1 * g
    v = 0.95 * v + 0.05 * g * g
    step = m * lax.rsqrt(v + 1e-8) + 0.1 * w
    return (w - 0.02 * step).astype(jnp.bfloat16), m, v


def clipped(gradients, sum_of_squares, count):
    factor = jnp.minimum(1.0, 0.5 * lax.rsqrt(sum_of_squares / count + 1e-30))
    return [g * factor for g in gradients]


def stack(weights, h):
    return lax.scan(lambda h, w: (layer(h, w), None), h, weights)[0]


def reference(x, dy, w_gate, w_up, w_down, m_w_gate, m_w_up, m_w_down, v_w_gate, v_w_up, v_w_down):
    weights = dict(zip(NAMES, (w_gate, w_up, w_down), strict=True))

    def take(so_far, sequence):
        h, by_y = sequence
        _, back = jax.vjp(lambda w: stack(w, h), weights)
        return jax.tree.map(lambda total, term: total + term.astype(jnp.float32), so_far, back(by_y)[0]), None

    none_yet = {name: jnp.zeros(w.shape, jnp.float32) for name, w in weights.items()}
    by_weights, _ = lax.scan(take, none_yet, (x, dy))
    gradients = [by_weights[name].astype(jnp.bfloat16).astype(jnp.float32) for name in NAMES]
    gradients = clipped(gradients, sum(jnp.sum(g * g) for g in gradients), sum(g.size for g in gradients))
    new = [
        adamw(w.astype(jnp.float32), m, v, g)
        for w, m, v, g in zip((w_gate, w_up, w_down), (m_w_gate, m_w_up, m_w_down), (v_w_gate, v_w_up, v_w_down), gradients, strict=True)
    ]
    return tuple(one[which] for which in range(3) for one in new)
```

```python
import functools
import math

import jax
import jax.numpy as jnp
from jax import lax
from jax.experimental import pallas as pl
from jax.experimental.pallas import tpu as pltpu
from jax.sharding import PartitionSpec as P

MESH = pl.DeviceIdType.MESH
F32, BF16 = jnp.float32, jnp.bfloat16
ANY = pl.BlockSpec(memory_space=pl.ANY)
HELD = pl.BlockSpec(memory_space=pltpu.VMEM)
TILE = 256
BLOCK = 256
UNIT = 16

LAGS = (0, 2, 4, 5, 7)


def schedule(numbers):
    for time in range(2 * numbers + LAGS[-1]):
        if time < 2 * numbers:
            yield 0, time // 2, time % 2
        for step, lag in reversed(list(enumerate(LAGS))):
            number, odd = divmod(time - lag - 1, 2)
            if not odd and 0 <= number < numbers:
                yield from ((step + 1, number, half) for half in (0, 1))


def normed(h):
    wide = h.astype(F32)
    scale = lax.rsqrt(jnp.mean(wide**2, -1, keepdims=True) + 1e-6)
    return (wide * scale).astype(BF16), scale


def sigmoid(x):
    return 0.5 * jnp.tanh(0.5 * x) + 0.5


def mm(a, b):
    return jnp.dot(a, b, preferred_element_type=F32)


def mm_t(a, b):
    return lax.dot_general(a, b, (((1,), (1,)), ((), ())), preferred_element_type=F32)


def token_kernel(layers, x_ref, dy_ref, w_gate, w_up, w_down, *refs):
    lhs, rhs, saved = refs[: 2 * layers], refs[2 * layers : 5 * layers], refs[5 * layers :]
    ff = w_gate.shape[2]
    pieces = [pl.ds(start, TILE) for start in range(0, ff, TILE)]
    h, dh = x_ref[...], dy_ref[...]
    states = []
    for l in range(layers):
        last = l + 1 == layers
        a, scale = normed(h)
        lhs[2 * l][...] = a.T
        states.append((h, scale))
        if last:
            lhs[2 * l + 1][...] = dh.T
        total = back_gate = back_up = None
        for piece in pieces:
            gate, up = mm(a, w_gate[l, :, piece]), mm(a, w_up[l, :, piece])
            s = sigmoid(gate)
            silu = gate * s
            act = (silu * up).astype(BF16)
            rhs[3 * l + 2][:, piece] = act
            slope = up * (s + silu * (1.0 - s))
            if last:
                dact = mm_t(dh, w_down[l, piece, :]).astype(BF16).astype(F32)
                dup, dgate = (dact * silu).astype(BF16), (dact * slope).astype(BF16)
                rhs[3 * l][:, piece], rhs[3 * l + 1][:, piece] = dgate, dup
                p, q = mm_t(dgate, w_gate[l, :, piece]), mm_t(dup, w_up[l, :, piece])
                back_gate = p if back_gate is None else back_gate + p
                back_up = q if back_up is None else back_up + q
            else:
                saved[2 * l][:, piece], saved[2 * l + 1][:, piece] = silu, slope
                p = mm(act, w_down[l, piece, :])
                total = p if total is None else total + p
        if not last:
            h = h + total.astype(BF16)
    for l in reversed(range(layers)):
        if l + 1 < layers:
            lhs[2 * l + 1][...] = dh.T
            back_gate = back_up = None
            for piece in pieces:
                dact = mm_t(dh, w_down[l, piece, :]).astype(BF16).astype(F32)
                dup, dgate = (dact * saved[2 * l][:, piece]).astype(BF16), (dact * saved[2 * l + 1][:, piece]).astype(BF16)
                rhs[3 * l][:, piece], rhs[3 * l + 1][:, piece] = dgate, dup
                if l:
                    p, q = mm_t(dgate, w_gate[l, :, piece]), mm_t(dup, w_up[l, :, piece])
                    back_gate = p if back_gate is None else back_gate + p
                    back_up = q if back_up is None else back_up + q
        if l:
            h, scale = states[l]
            da = (back_gate.astype(BF16) + back_up.astype(BF16)).astype(F32)
            wide = h.astype(F32)
            along = jnp.mean(da * wide, -1, keepdims=True)
            dh = dh + (da * scale - wide * (scale * scale * scale * along)).astype(BF16)


def token_phase(x, dy, ws):
    layers, d, ff = ws[0].shape
    tokens = x.shape[0]
    block = min(BLOCK, tokens)
    whole = [pl.BlockSpec(w.shape, lambda i: (0, 0, 0), pipeline_mode=pl.Buffered(1)) for w in ws]
    rows = lambda width: pl.BlockSpec((block, width), lambda i: (i, 0))
    outs = [jax.ShapeDtypeStruct((d, tokens), BF16)] * (2 * layers) + [jax.ShapeDtypeStruct((tokens, ff), BF16)] * (3 * layers)
    products = 9 if layers == 2 else 8 * layers
    got = pl.pallas_call(
        functools.partial(token_kernel, layers),
        grid=(tokens // block,),
        out_shape=outs,
        in_specs=[rows(d), rows(d), *whole],
        out_specs=[pl.BlockSpec((d, block), lambda i: (0, i))] * (2 * layers) + [rows(ff)] * (3 * layers),
        scratch_shapes=[pltpu.VMEM((block, ff), F32)] * (2 * (layers - 1)),
        compiler_params=pltpu.CompilerParams(vmem_limit_bytes=60 * 2**20),
        cost_estimate=pl.CostEstimate(flops=2 * products * tokens * d * ff, bytes_accessed=2 * 6 * tokens * ff, transcendentals=0),
    )(x, dy, *ws)
    return got[: 2 * layers], got[2 * layers :]


def write_kernel(*refs):
    sources, targets, sem = refs[:9], refs[9:18], refs[18]
    copies = [
        pltpu.make_async_copy(source.at[l], target.at[l], sem.at[i, l])
        for i, (source, target) in enumerate(zip(sources, targets)) for l in range(source.shape[0])
    ]
    for copy in copies:
        copy.start()
    for copy in copies:
        copy.wait()


class Spot:
    def __init__(self, side):
        self.side = side
        me = lax.axis_index("dp")
        self.me, self.at = me, (me // side, me % side)

    def along(self, axis, by):
        return (self.at[axis] + by) % self.side

    def device(self, axis, by):
        x, y = (self.along(a, by) if a == axis else self.at[a] for a in (0, 1))
        return {"dp": x * self.side + y}


def kernel(side, layers, kinds, count, *refs):
    refs = list(refs)
    take = lambda k: [refs.pop(0) for _ in range(k)]
    lhs_in = take(2 * layers)
    rhs_in = take(3 * layers)
    w_in, m_in, v_in = take(3), take(3), take(3)
    terms = take(3)
    m, v = take(3), take(3)
    lhs, rhs = take(2)
    far1, near1, far2, near2, own = (take(3) for _ in range(5))
    grad, w, new = (take(3) for _ in range(3))
    squares = take(1)[0]
    lhs_sem, rhs_sem, io_sem, ssem, rsem, ex_ssem, ex_rsem, ag_ssem, ag_rsem = take(9)
    assert not refs

    spot = Spot(side)
    half_ring = side // 2
    order = [(kind, layer) for layer in reversed(range(layers)) for kind in (0, 1, 2)]

    loads = []
    lhs_loads = {}
    for layer in reversed(range(layers)):
        for which in (0, 1):
            i = 2 * layer + which
            lhs_loads[i] = pltpu.make_async_copy(lhs_in[i], lhs.at[i], lhs_sem.at[i])

    tiles = rhs_in[0].shape[1] // TILE

    def rhs_load(number, tile):
        kind, layer = order[number]
        slot = (number * tiles + tile) % 2
        columns = pl.ds(pl.multiple_of(tile * TILE, TILE), TILE)
        return pltpu.make_async_copy(rhs_in[3 * layer + kind].at[:, columns], rhs.at[slot], rhs_sem.at[slot])

    lhs_loads[2 * (layers - 1)].start()
    rhs_load(0, 0).start()
    for i, load in lhs_loads.items():
        if i != 2 * (layers - 1):
            load.start()
    for kind in range(3):
        rows = kinds[kind][0]
        mine = pl.ds(pl.multiple_of(spot.me * rows, UNIT), rows)
        loads.append(pltpu.make_async_copy(w_in[kind].at[:, mine, :], w[kind], io_sem.at[kind]))
        loads.append(pltpu.make_async_copy(m_in[kind], m[kind], io_sem.at[3 + kind]))
        loads.append(pltpu.make_async_copy(v_in[kind], v[kind], io_sem.at[6 + kind]))
    for load in loads:
        load.start()

    barrier = pltpu.get_barrier_semaphore()
    for axis in (0, 1):
        for by in range(1, side):
            pl.semaphore_signal(barrier, inc=1, device_id=spot.device(axis, by), device_id_type=MESH)
    pl.semaphore_wait(barrier, 2 * (side - 1))

    sent = []

    def send(src, dst, sems, index, device):
        copy = pltpu.make_async_remote_copy(
            src_ref=src, dst_ref=dst, send_sem=sems[0].at[index], recv_sem=sems[1].at[index],
            device_id=device, device_id_type=MESH)
        copy.start()
        sent.append(copy)
        return copy

    ready = set()
    parts = [(0, -(-tiles // 2)), (-(-tiles // 2), tiles)]

    def compute(number, part):
        kind, layer = order[number]
        i = 2 * layer + (kind == 2)
        if i not in ready:
            ready.add(i)
            lhs_loads[i].wait()
        term = terms[kind].at[layer]
        rows, columns = kinds[kind]

        def body(tile, carry):
            slot = (number * tiles + tile) % 2
            rhs_load(number, tile).wait()

            @pl.when(tile + 1 < tiles)
            def _():
                rhs_load(number, tile + 1).start()

            if number + 1 < len(order):
                @pl.when(tile + 1 == tiles)
                def _():
                    rhs_load(number + 1, 0).start()

            product = jnp.dot(lhs[i], rhs[slot], preferred_element_type=F32).astype(BF16)
            if kind < 2:
                here = pl.ds(pl.multiple_of(tile * TILE, TILE), TILE)
                term[:, :, :, here] = product.reshape(side, side, rows, TILE)
            else:
                turned = product.T
                for unit in range(TILE // UNIT):
                    place = tile * (TILE // UNIT) + unit
                    block, row = place // (rows // UNIT), place % (rows // UNIT)
                    term[block // side, block % side, pl.ds(pl.multiple_of(row * UNIT, UNIT), UNIT), :] = (
                        turned[unit * UNIT : (unit + 1) * UNIT])
            return carry

        lax.fori_loop(*parts[part], body, 0)

    class Sum:
        def __init__(self, number, half):
            self.kind, self.layer = order[number]
            self.rows, columns = kinds[self.kind]
            self.width = columns // 2
            self.columns = pl.ds(half * self.width, self.width)
            self.first, self.second, self.half = half, 1 - half, half
            self.term = terms[self.kind].at[self.layer]
            self.base = 8 * (2 * number + half)
            cut = UNIT * (self.rows // UNIT // 2 + (number + half) % 2 * (self.rows // UNIT % 2))
            self.cuts = (pl.ds(0, cut), pl.ds(cut, self.rows - cut))
            b = (self.layer, half)
            self.far1, self.near1, self.far2, self.near2, self.own = (r[self.kind].at[b] for r in (far1, near1, far2, near2, own))
            self.copies = {}

        def block(self, first, second):
            return (first, second) if self.half == 0 else (second, first)

        def go(self, event, way, src, dst, axis):
            sems = (ssem, rsem)
            self.copies[event, way] = send(src, dst, sems, self.base + 2 * event + way, spot.device(axis, 1 - 2 * way))

        def arrived(self, event):
            for way in (0, 1):
                self.copies[event, way].wait_recv()

        def each(self, work):
            def body(unit, carry):
                work(pl.ds(pl.multiple_of(unit * UNIT, UNIT), UNIT))
                return carry
            lax.fori_loop(0, self.rows // UNIT, body, 0)

        def step1(self):
            away = spot.along(self.first, half_ring)
            for way in (0, 1):
                some = pl.ds(way * half_ring, half_ring)
                src = self.term.at[self.block(away, some) + (slice(None), self.columns)]
                self.go(0, way, src, self.far1.at[way], self.first)

        def step2(self):
            self.arrived(0)
            for way in (0, 1):
                to = spot.along(self.first, 1 - 2 * way)

                def work(rows):
                    for j in range(half_ring):
                        at = self.block(to, way * half_ring + j) + (rows, self.columns)
                        total = self.term[at].astype(F32) + self.far1[way, j, rows, :].astype(F32)
                        self.term[at] = total.astype(BF16)

                self.each(work)
                src = self.term.at[self.block(to, slice(None)) + (slice(None), self.columns)]
                self.go(1, way, src, self.near1.at[way], self.first)

        def step3(self):
            self.arrived(1)
            me = spot.at[self.first]

            def total(second, rows):
                at = self.block(me, second) + (rows, self.columns)
                return (self.term[at].astype(F32) + self.near1[0, second, rows, :].astype(F32)) + self.near1[1, second, rows, :].astype(F32)

            def work(rows):
                for by in range(1, side):
                    second = spot.along(self.second, by)
                    self.term[self.block(me, second) + (rows, self.columns)] = total(second, rows).astype(BF16)
                self.own[rows, :] = total(spot.at[self.second], rows)

            self.each(work)
            away = spot.along(self.second, half_ring)
            for way in (0, 1):
                src = self.term.at[self.block(me, away) + (self.cuts[way], self.columns)]
                self.go(2, way, src, self.far2.at[self.cuts[way]], self.second)

        def step4(self):
            self.arrived(2)
            me = spot.at[self.first]
            for way in (0, 1):
                to = spot.along(self.second, 1 - 2 * way)
                at = self.block(me, to) + (self.cuts[way], self.columns)
                self.term[at] = (self.term[at].astype(F32) + self.far2[self.cuts[way]].astype(F32)).astype(BF16)
                src = self.term.at[self.block(me, to) + (slice(None), self.columns)]
                self.go(3, way, src, self.near2.at[way], self.second)

        def step5(self):
            self.arrived(3)

            def work(rows):
                total = (self.own[rows, :] + self.near2[0, rows, :].astype(F32)) + self.near2[1, rows, :].astype(F32)
                grad[self.kind][self.layer, rows, self.columns] = total.astype(BF16)

            self.each(work)

    sums = {(number, half): Sum(number, half) for number in range(len(order)) for half in (0, 1)}
    for what, number, which in schedule(len(order)):
        if what == 0:
            compute(number, which)
        else:
            getattr(sums[number, which], f"step{what}")()

    for copy in sent:
        copy.wait_send()
    sent.clear()

    part = jnp.zeros((8, 128), F32)
    for kind in range(3):
        rows, columns = kinds[kind]
        for layer in range(layers):
            def body(unit, part):
                g = grad[kind][layer, pl.ds(pl.multiple_of(unit * UNIT, UNIT), UNIT), :].astype(F32)
                g = g * g
                for i in range(UNIT // 8):
                    for j in range(columns // 128):
                        part = part + g[8 * i : 8 * i + 8, 128 * j : 128 * j + 128]
                return part
            part = lax.fori_loop(0, rows // UNIT, body, part)
    for axis in (0, 1):
        mine = spot.at[axis]
        squares[axis, mine] = part
        for by in range(1, side):
            copy = pltpu.make_async_remote_copy(
                src_ref=squares.at[axis, mine], dst_ref=squares.at[axis, mine], send_sem=ex_ssem.at[axis, by], recv_sem=ex_rsem.at[axis, mine],
                device_id=spot.device(axis, by), device_id_type=MESH)
            copy.start()
            sent.append(copy)
        for by in range(1, side):
            other = spot.along(axis, by)
            pltpu.make_async_remote_copy(
                src_ref=squares.at[axis, other], dst_ref=squares.at[axis, other], send_sem=ex_ssem.at[axis, by], recv_sem=ex_rsem.at[axis, other],
                device_id=spot.device(axis, by), device_id_type=MESH).wait_recv()
        part = squares[axis, 0]
        for i in range(1, side):
            part = part + squares[axis, i]
    total = jnp.sum(jnp.sum(part, 0, keepdims=True), 1, keepdims=True)
    factor = jnp.minimum(1.0, 0.5 * lax.rsqrt(total / count + 1e-30))

    for load in loads:
        load.wait()
    for kind in range(3):
        rows, columns = kinds[kind]

        def body(unit, carry):
            layer, unit = unit // (rows // UNIT), unit % (rows // UNIT)
            at = (layer, pl.ds(pl.multiple_of(unit * UNIT, UNIT), UNIT), slice(None))
            g = grad[kind][at].astype(F32) * factor
            m1 = 0.9 * m[kind][at] + 0.1 * g
            v1 = 0.95 * v[kind][at] + 0.05 * g * g
            wide = w[kind][at].astype(F32)
            m[kind][at], v[kind][at] = m1, v1
            fresh = (wide - 0.02 * (m1 * lax.rsqrt(v1 + 1e-8) + 0.1 * wide)).astype(BF16)
            new[kind][at] = fresh
            terms[kind][(layer, *spot.at, *at[1:])] = fresh
            return carry

        lax.fori_loop(0, layers * (rows // UNIT), body, 0)

    class Gather:
        def __init__(self, half, kind):
            self.half, self.kind = half, kind
            self.rows, columns = kinds[kind]
            self.columns = pl.ds(half * (columns // 2), columns // 2)
            self.first, self.second = half, 1 - half
            self.base = 20 * (3 * half + kind)

        def place(self, by_first, by_second, some=slice(None)):
            a, b = spot.along(self.first, by_first), spot.along(self.second, by_second)
            x, y = (a, b) if self.half == 0 else (b, a)
            return terms[self.kind].at[some, x, y, :, self.columns]

        def go(self, index, way, axis, at, src=None):
            send(at if src is None else src, at, (ag_ssem, ag_rsem), self.base + index + way, spot.device(axis, 1 - 2 * way))

        def arrived(self, index, way, at):
            pltpu.make_async_remote_copy(
                src_ref=at, dst_ref=at, send_sem=ag_ssem.at[self.base + index + way], recv_sem=ag_rsem.at[self.base + index + way],
                device_id=spot.device(0, 1), device_id_type=MESH).wait_recv()

        def some(self, way):
            return pl.ds(way * (layers // 2), layers // 2)

        def start(self):
            src = new[self.kind].at[:, :, self.columns]
            for way in (0, 1):
                self.go(0, way, self.first, self.place(0, 0), src)
            for way in (0, 1):
                self.go(4, way, self.second, self.place(0, 0), src)

        def first_near(self, way):
            by = 2 * way - 1
            self.arrived(0, way, self.place(by, 0))
            self.go(2, way, self.first, self.place(by, 0, self.some(way)))
            for to in (0, 1):
                self.go(8 + 4 * way, to, self.second, self.place(by, 0))

        def first_far(self):
            for way in (0, 1):
                self.arrived(2, way, self.place(half_ring, 0, self.some(way)))
            for to in (0, 1):
                self.go(16, to, self.second, self.place(half_ring, 0))

        def second_near(self, which):
            by_first = (0, -1, 1, half_ring)[which]
            for way in (0, 1):
                by = 2 * way - 1
                self.arrived(4 + 4 * which, way, self.place(by_first, by))
                self.go(6 + 4 * which, way, self.second, self.place(by_first, by, self.some(way)))

        def second_far(self, which):
            by_first = (0, -1, 1, half_ring)[which]
            for way in (0, 1):
                self.arrived(6 + 4 * which, way, self.place(by_first, half_ring, self.some(way)))

    gathers = [Gather(half, kind) for kind in range(3) for half in (0, 1)]
    for gather in gathers:
        gather.start()
    for way in (0, 1):
        for gather in gathers:
            gather.first_near(way)
    for gather in gathers:
        gather.second_near(0)
    for gather in gathers:
        gather.first_far()
    for which in (1, 2, 3):
        for gather in gathers:
            gather.second_near(which)
    for which in range(4):
        for gather in gathers:
            gather.second_far(which)
    for copy in sent:
        copy.wait_send()


def solution(mesh):
    n = mesh.shape["dp"]
    side = math.isqrt(n)

    def update(lhs, rhs, ws, ms, vs):
        layers = ws[0].shape[0]
        d, tokens = lhs[0].shape
        kinds = tuple((m.shape[1], m.shape[2]) for m in ms)
        count = float(sum(w.size for w in ws))
        scratch = [pltpu.VMEM((2 * layers, d, tokens), BF16), pltpu.VMEM((2, tokens, TILE), BF16)]
        scratch += [pltpu.VMEM((layers, 2, 2, side // 2, r, c // 2), BF16) for r, c in kinds]
        scratch += [pltpu.VMEM((layers, 2, 2, side, r, c // 2), BF16) for r, c in kinds]
        scratch += [pltpu.VMEM((layers, 2, r, c // 2), BF16) for r, c in kinds]
        scratch += [pltpu.VMEM((layers, 2, 2, r, c // 2), BF16) for r, c in kinds]
        scratch += [pltpu.VMEM((layers, 2, r, c // 2), F32) for r, c in kinds]
        for dtype in (BF16, BF16, BF16):
            scratch += [pltpu.VMEM((layers, r, c), dtype) for r, c in kinds]
        scratch += [pltpu.VMEM((2, side, 8, 128), F32)]
        dma = pltpu.SemaphoreType.DMA
        sums, gathers = 8 * 2 * 3 * layers, 20 * 6
        scratch += [dma((2 * layers,)), dma((2,)), dma((9,)), dma((sums,)), dma((sums,)),
                    dma((2, side)), dma((2, side)), dma((gathers,)), dma((gathers,))]
        got = pl.pallas_call(
            functools.partial(kernel, side, layers, kinds, count),
            out_shape=[pltpu.VMEM((layers, side, side, r, c), BF16) for r, c in kinds] + [pltpu.VMEM(m.shape, F32) for m in (*ms, *vs)],
            in_specs=[ANY] * (len(lhs) + len(rhs) + 9),
            out_specs=[HELD] * 9,
            scratch_shapes=scratch,
            compiler_params=pltpu.CompilerParams(collective_id=0, has_side_effects=True, vmem_limit_bytes=40 * 2**20),
        )(*lhs, *rhs, *ws, *ms, *vs)
        out = pl.pallas_call(
            write_kernel,
            out_shape=[jax.ShapeDtypeStruct(t.shape, t.dtype) for t in got],
            in_specs=[HELD] * 9,
            out_specs=[ANY] * 9,
            scratch_shapes=[dma((9, layers))],
            compiler_params=pltpu.CompilerParams(vmem_limit_bytes=4 * 2**20),
        )(*got)
        return [t.reshape(w.shape) for t, w in zip(out, (*ws, *ms, *vs))]

    def step(x, dy, *arrays):
        ws, ms, vs = (arrays[i : i + 3] for i in (0, 3, 6))
        lhs, rhs = token_phase(x[0], dy[0], ws)
        return tuple(update(lhs, rhs, ws, ms, vs))

    data, whole, rows = P(("rep", "dp")), P(), P(None, "dp")
    return jax.shard_map(
        step, mesh=mesh,
        in_specs=(data, data, whole, whole, whole) + (rows,) * 6,
        out_specs=(P("rep"),) * 3 + (P("rep", "dp"),) * 6,
        check_vma=False,
    )
```

```python
import functools
import math

import jax
import jax.numpy as jnp
from jax import lax
from jax.experimental import pallas as pl
from jax.experimental.pallas import tpu as pltpu
from jax.sharding import PartitionSpec as P

MESH = pl.DeviceIdType.MESH
F32, BF16 = jnp.float32, jnp.bfloat16
ANY = pl.BlockSpec(memory_space=pl.ANY)
HELD = pl.BlockSpec(memory_space=pltpu.VMEM)
TILE = 256
BLOCK = 256
UNIT = 16

ORDER = ((0, 1), (1, 1), (2, 1), (2, 0), (0, 0), (1, 0))
SEGMENTS = 4
HALF, PIECE, LATENCY = 3.6, 9.0, 2.3
WORK, WIRE = (0.1, 0.7, 1.0, 0.3, 0.4), (3.6, 7.2, 0.9, 1.8)


def schedule():
    turn = [i for i in range(1, len(ORDER)) if ORDER[i][1] != ORDER[i - 1][1]][0]
    products = [(0, number, half) for number in range(len(ORDER)) for half in (0, 1)]
    products[2 * turn : 2 * turn] = [(6, 0, piece) for piece in range(SEGMENTS)]
    now, free, due, done = 2.0, [0.0, 0.0], {}, set()

    def may(event):
        step, number, half = event
        kind = ORDER[number][0]
        if step == 1:
            return all((5, other, i) in done for other in range(number) if ORDER[other][0] == kind for i in (0, 1))
        return step != 4 or all((3, number, i) in done for i in (0, 1))

    while products or due:
        can = [event for event in due if may(event)]
        here = [event for event in can if due[event] <= now]
        if here:
            event = min(here)
        elif products:
            event = products.pop(0)
        else:
            event = min(can, key=lambda event: (due[event], event))
        step, number, half = event
        if step == 6:
            now += PIECE
        elif step == 0:
            now += HALF
            for i in (0, 1):
                if half == i if ORDER[number][0] < 2 else half:
                    due[1, number, i] = now
        else:
            now = max(now, due.pop(event)) + WORK[step - 1]
            if step < 5:
                axis = half if step < 3 else 1 - half
                free[axis] = max(free[axis], now) + WIRE[step - 1]
                due[step + 1, number, half] = free[axis] + LATENCY
        done.add(event)
        yield event


def normed(h):
    wide = h.astype(F32)
    scale = lax.rsqrt(jnp.mean(wide**2, -1, keepdims=True) + 1e-6)
    return (wide * scale).astype(BF16), scale


def sigmoid(x):
    return 0.5 * jnp.tanh(0.5 * x) + 0.5


def mm(a, b):
    return jnp.dot(a, b, preferred_element_type=F32)


def mm_t(a, b):
    return lax.dot_general(a, b, (((1,), (1,)), ((), ())), preferred_element_type=F32)


def token_kernel(x_ref, dy_ref, w_gate, w_up, w_down, a_first, a_last, turned_dy, act_first, dgate, dup, act_last, silu_first, slope_first, h_last):
    pieces = [pl.ds(start, TILE) for start in range(0, w_gate.shape[2], TILE)]
    dh = dy_ref[...]
    turned_dy[...] = dh.T
    h = x_ref[...]
    a, _ = normed(h)
    a_first[...] = a.T
    total = None
    for piece in pieces:
        gate, up = mm(a, w_gate[0, :, piece]), mm(a, w_up[0, :, piece])
        silu, slope = slopes(gate, up)
        act = (silu * up).astype(BF16)
        act_first[:, piece], silu_first[:, piece], slope_first[:, piece] = act, silu, slope
        p = mm(act, w_down[0, piece, :])
        total = p if total is None else total + p
    h = h + total.astype(BF16)
    h_last[...] = h
    a, _ = normed(h)
    a_last[...] = a.T
    for piece in pieces:
        gate, up = mm(a, w_gate[1, :, piece]), mm(a, w_up[1, :, piece])
        silu, slope = slopes(gate, up)
        act_last[:, piece] = (silu * up).astype(BF16)
        dact = mm_t(dh, w_down[1, piece, :]).astype(BF16).astype(F32)
        dgate[:, piece], dup[:, piece] = (dact * slope).astype(BF16), (dact * silu).astype(BF16)


def slopes(gate, up):
    s = sigmoid(gate)
    silu = gate * s
    return silu, up * (s + silu * (1.0 - s))


def token_phase(x, dy, ws):
    _, d, ff = ws[0].shape
    tokens = x.shape[0]
    block = min(BLOCK, tokens)
    whole = [pl.BlockSpec(w.shape, lambda i: (0, 0, 0), pipeline_mode=pl.Buffered(1)) for w in ws]
    rows = lambda width: pl.BlockSpec((block, width), lambda i: (i, 0))
    turned = pl.BlockSpec((d, block), lambda i: (0, i))
    shape = jax.ShapeDtypeStruct
    return pl.pallas_call(
        token_kernel,
        grid=(tokens // block,),
        out_shape=[shape((d, tokens), BF16)] * 3 + [shape((tokens, ff), BF16)] * 4 + [shape((tokens, ff), F32)] * 2 + [shape((tokens, d), BF16)],
        in_specs=[rows(d), rows(d), *whole],
        out_specs=[turned] * 3 + [rows(ff)] * 6 + [rows(d)],
        compiler_params=pltpu.CompilerParams(vmem_limit_bytes=64 * 2**20 - 2**16),
        cost_estimate=pl.CostEstimate(flops=12 * tokens * d * ff, bytes_accessed=24 * tokens * ff, transcendentals=0),
    )(x, dy, *ws)


def write_kernel(*refs):
    sources, targets, sem = refs[:9], refs[9:18], refs[18]
    copies = [
        pltpu.make_async_copy(source.at[l], target.at[l], sem.at[i, l])
        for i, (source, target) in enumerate(zip(sources, targets)) for l in range(source.shape[0])
    ]
    for copy in copies:
        copy.start()
    for copy in copies:
        copy.wait()


class Spot:
    def __init__(self, side):
        self.side = side
        me = lax.axis_index("dp")
        self.me, self.at = me, (me // side, me % side)

    def along(self, axis, by):
        return (self.at[axis] + by) % self.side

    def device(self, axis, by):
        x, y = (self.along(a, by) if a == axis else self.at[a] for a in (0, 1))
        return {"dp": x * self.side + y}


def kernel(side, kinds, count, *refs):
    refs = list(refs)
    take = lambda k: [refs.pop(0) for _ in range(k)]
    a_first, a_last, turned_dy, act_first, dgate_last, dup_last, act_last, silu_in, slope_in, h_in, dy_in = take(11)
    w_in, m_in, v_in = take(3), take(3), take(3)
    terms = take(3)
    m, v = take(3), take(3)
    dgate_first, dup_first = take(2)
    lhs, rhs, down = take(3)
    dgate_buf, dup_buf, silu_buf, slope_buf, h_buf, dy_buf, dgate_new, dup_new = take(8)
    far1, near1, far2, near2, own = (take(3) for _ in range(5))
    grad, w = take(3), take(3)
    squares = take(1)[0]
    lhs_sem, rhs_sem, w_sem, block_sem, io_sem, ssem, rsem, ex_ssem, ex_rsem, ag_ssem, ag_rsem = take(11)
    assert not refs
    layers = terms[0].shape[0]
    rhs_in = {(0, 1): dgate_last, (1, 1): dup_last, (2, 1): act_last, (2, 0): act_first, (0, 0): dgate_first, (1, 0): dup_first}
    order = ORDER

    spot = Spot(side)
    half_ring = side // 2

    size = h_buf.shape[0]
    blocks = h_in.shape[0] // size
    pairs = (
        ((dgate_last, dgate_buf), (dup_last, dup_buf)),
        ((h_in, h_buf), (dy_in, dy_buf), (silu_in, silu_buf), (slope_in, slope_buf)),
        ((dgate_first, dgate_new), (dup_first, dup_new)),
    )

    def block_loads(stage, block):
        here = pl.ds(pl.multiple_of(block * size, size), size)
        return [pltpu.make_async_copy(far.at[here, :], near, block_sem.at[stage, i]) for i, (far, near) in enumerate(pairs[stage])]

    def block_stores(block):
        here = pl.ds(pl.multiple_of(block * size, size), size)
        return [pltpu.make_async_copy(near, far.at[here, :], block_sem.at[2, i]) for i, (far, near) in enumerate(pairs[2])]

    def weight_loads(kind):
        return [
            pltpu.make_async_copy(w_in[kind].at[1, :, pl.ds(i * width, width)], rhs.at[kind, pl.ds(i * d, d), :], w_sem.at[2 * kind + i])
            for i in (0, 1)
        ]

    def back(kind, buf):
        return sum(mm_t(buf[:, i * width : (i + 1) * width], rhs[kind, i * d : (i + 1) * d, :]) for i in (0, 1)).astype(BF16)

    def tokens_backward(piece):
        if piece == 0:
            for kind in (0, 1):
                for load in weight_loads(kind):
                    load.wait()
            load_down.wait()

        def body(block, carry):
            for load in block_loads(0, block):
                load.wait()
            da = (back(0, dgate_buf) + back(1, dup_buf)).astype(F32)

            @pl.when(block + 1 < blocks)
            def _():
                for load in block_loads(0, block + 1):
                    load.start()

            @pl.when(block + 1 == blocks)
            def _():
                rhs_load(3, 0).start()

            for load in block_loads(1, block):
                load.wait()
            h = h_buf[...]
            _, scale = normed(h)
            wide = h.astype(F32)
            along = jnp.mean(da * wide, -1, keepdims=True)
            dh = dy_buf[...] + (da * scale - wide * (scale * scale * scale * along)).astype(BF16)
            lhs[1, :, pl.ds(pl.multiple_of(block * size, size), size)] = dh.T

            @pl.when(block > 0)
            def _():
                for store in block_stores(block - 1):
                    store.wait()

            for start in range(0, 2 * width, TILE):
                some = pl.ds(start, TILE)
                dact = mm_t(dh, down[some, :]).astype(BF16).astype(F32)
                dgate_new[:, some], dup_new[:, some] = (dact * slope_buf[:, some]).astype(BF16), (dact * silu_buf[:, some]).astype(BF16)
            for store in block_stores(block):
                store.start()

            @pl.when(block + 1 < blocks)
            def _():
                for load in block_loads(1, block + 1):
                    load.start()

            return carry

        lax.fori_loop(piece * blocks // SEGMENTS, (piece + 1) * blocks // SEGMENTS, body, 0)
        if piece + 1 == SEGMENTS:
            for store in block_stores(blocks - 1):
                store.wait()

    loads = []
    width = rhs.shape[2]
    d = lhs.shape[1]

    def rhs_load(number, part):
        return pltpu.make_async_copy(rhs_in[order[number]].at[:, pl.ds(part * width, width)], rhs.at[part], rhs_sem.at[part])

    load_a_last = pltpu.make_async_copy(a_last, lhs.at[0], lhs_sem.at[0])
    load_dy = pltpu.make_async_copy(turned_dy, lhs.at[1], lhs_sem.at[1])
    load_a_first = pltpu.make_async_copy(a_first, lhs.at[0], lhs_sem.at[2])
    load_down = pltpu.make_async_copy(w_in[2].at[0], down, w_sem.at[4])
    load_a_last.start()
    rhs_load(0, 0).start()
    load_dy.start()
    load_down.start()
    for load in (*block_loads(0, 0), *block_loads(1, 0)):
        load.start()
    for kind in range(3):
        rows = kinds[kind][0]
        mine = pl.ds(pl.multiple_of(spot.me * rows, UNIT), rows)
        loads.append(pltpu.make_async_copy(w_in[kind].at[:, mine, :], w[kind], io_sem.at[kind]))
        loads.append(pltpu.make_async_copy(m_in[kind], m[kind], io_sem.at[3 + kind]))
        loads.append(pltpu.make_async_copy(v_in[kind], v[kind], io_sem.at[6 + kind]))
    for load in loads:
        load.start()

    barrier = pltpu.get_barrier_semaphore()
    for axis in (0, 1):
        for by in range(1, side):
            pl.semaphore_signal(barrier, inc=1, device_id=spot.device(axis, by), device_id_type=MESH)
    pl.semaphore_wait(barrier, 2 * (side - 1))

    sent = []

    def send(src, dst, sems, index, device):
        copy = pltpu.make_async_remote_copy(
            src_ref=src, dst_ref=dst, send_sem=sems[0].at[index], recv_sem=sems[1].at[index],
            device_id=device, device_id_type=MESH)
        copy.start()
        sent.append(copy)
        return copy

    def compute(number, part):
        kind, layer = order[number]
        which = kind // 2
        term = terms[kind].at[layer]
        rows, columns = kinds[kind]
        if part == 0 and (number == 0 or number == 2 or number == 4):
            {0: load_a_last, 2: load_dy, 4: load_a_first}[number].wait()
        rhs_load(number, part).wait()
        if part == 0:
            rhs_load(number, 1).start()
        elif number + 1 < len(order) and number != 2:
            rhs_load(number + 1, 0).start()
        deep = d // 2

        def body(half, carry):
            some = pl.ds(pl.multiple_of(half * deep, deep), deep)
            product = jnp.dot(lhs[which, some, :], rhs[part], preferred_element_type=F32).astype(BF16)
            if kind < 2:
                term[pl.ds(half * half_ring, half_ring), :, :, pl.ds(part * width, width)] = product.reshape(half_ring, side, rows, width)
            else:
                term[pl.ds(part * half_ring, half_ring), :, :, some] = product.T.reshape(half_ring, side, rows, deep)
            return carry

        lax.fori_loop(0, 2, body, 0)
        if number == 1 and part:
            load_a_first.start()
        if number == 2:
            for load in weight_loads(part):
                load.start()

    class Sum:
        def __init__(self, number, half):
            self.kind, self.layer = order[number]
            self.rows, columns = kinds[self.kind]
            self.width = columns // 2
            self.columns = pl.ds(half * self.width, self.width)
            self.first, self.second, self.half = half, 1 - half, half
            self.term = terms[self.kind].at[self.layer]
            self.base = 8 * (2 * number + half)
            cut = UNIT * (self.rows // UNIT // 2 + (number + half) % 2 * (self.rows // UNIT % 2))
            self.cuts = (pl.ds(0, cut), pl.ds(cut, self.rows - cut))
            self.far1, self.near1 = far1[self.kind].at[half], near1[self.kind].at[half]
            self.far2, self.near2, self.own = (r[self.kind].at[self.layer, half] for r in (far2, near2, own))
            self.copies = {}

        def block(self, first, second):
            return (first, second) if self.half == 0 else (second, first)

        def go(self, event, way, src, dst, axis):
            sems = (ssem, rsem)
            self.copies[event, way] = send(src, dst, sems, self.base + 2 * event + way, spot.device(axis, 1 - 2 * way))

        def arrived(self, event):
            for way in (0, 1):
                self.copies[event, way].wait_recv()

        def each(self, work):
            def body(unit, carry):
                work(pl.ds(pl.multiple_of(unit * UNIT, UNIT), UNIT))
                return carry
            lax.fori_loop(0, self.rows // UNIT, body, 0)

        def step1(self):
            away = spot.along(self.first, half_ring)
            for way in (0, 1):
                some = pl.ds(way * half_ring, half_ring)
                src = self.term.at[self.block(away, some) + (slice(None), self.columns)]
                self.go(0, way, src, self.far1.at[way], self.first)

        def step2(self):
            self.arrived(0)
            for way in (0, 1):
                to = spot.along(self.first, 1 - 2 * way)

                def work(rows):
                    for j in range(half_ring):
                        at = self.block(to, way * half_ring + j) + (rows, self.columns)
                        total = self.term[at].astype(F32) + self.far1[way, j, rows, :].astype(F32)
                        self.term[at] = total.astype(BF16)

                self.each(work)
                src = self.term.at[self.block(to, slice(None)) + (slice(None), self.columns)]
                self.go(1, way, src, self.near1.at[way], self.first)

        def step3(self):
            self.arrived(1)
            me = spot.at[self.first]

            def total(second, rows):
                at = self.block(me, second) + (rows, self.columns)
                return (self.term[at].astype(F32) + self.near1[0, second, rows, :].astype(F32)) + self.near1[1, second, rows, :].astype(F32)

            def work(rows):
                for by in range(1, side):
                    second = spot.along(self.second, by)
                    self.term[self.block(me, second) + (rows, self.columns)] = total(second, rows).astype(BF16)
                self.own[rows, :] = total(spot.at[self.second], rows)

            self.each(work)
            away = spot.along(self.second, half_ring)
            for way in (0, 1):
                src = self.term.at[self.block(me, away) + (self.cuts[way], self.columns)]
                self.go(2, way, src, self.far2.at[self.cuts[way]], self.second)

        def step4(self):
            self.arrived(2)
            me = spot.at[self.first]
            for way in (0, 1):
                to = spot.along(self.second, 1 - 2 * way)
                at = self.block(me, to) + (self.cuts[way], self.columns)
                self.term[at] = (self.term[at].astype(F32) + self.far2[self.cuts[way]].astype(F32)).astype(BF16)
                src = self.term.at[self.block(me, to) + (slice(None), self.columns)]
                self.go(3, way, src, self.near2.at[way], self.second)

        def step5(self):
            self.arrived(3)

            def work(rows):
                total = (self.own[rows, :] + self.near2[0, rows, :].astype(F32)) + self.near2[1, rows, :].astype(F32)
                grad[self.kind][self.layer, rows, self.columns] = total.astype(BF16)

            self.each(work)

    sums = {(number, half): Sum(number, half) for number in range(len(order)) for half in (0, 1)}
    for what, number, which in schedule():
        if what == 0:
            compute(number, which)
        elif what == 6:
            tokens_backward(which)
        else:
            getattr(sums[number, which], f"step{what}")()

    for copy in sent:
        copy.wait_send()
    sent.clear()

    part = jnp.zeros((8, 128), F32)
    for kind in range(3):
        rows, columns = kinds[kind]
        for layer in range(layers):
            def body(unit, part):
                g = grad[kind][layer, pl.ds(pl.multiple_of(unit * UNIT, UNIT), UNIT), :].astype(F32)
                g = g * g
                tiles = [g[8 * i : 8 * i + 8, 128 * j : 128 * j + 128] for i in range(UNIT // 8) for j in range(columns // 128)]
                while len(tiles) > 1:
                    tiles = [sum(tiles[i + 1 : i + 2], tiles[i]) for i in range(0, len(tiles), 2)]
                part = part + tiles[0]
                return part
            part = lax.fori_loop(0, rows // UNIT, body, part)
    for axis in (0, 1):
        mine = spot.at[axis]
        squares[axis, mine] = part
        for by in range(1, side):
            copy = pltpu.make_async_remote_copy(
                src_ref=squares.at[axis, mine], dst_ref=squares.at[axis, mine], send_sem=ex_ssem.at[axis, by], recv_sem=ex_rsem.at[axis, mine],
                device_id=spot.device(axis, by), device_id_type=MESH)
            copy.start()
            sent.append(copy)
        for by in range(1, side):
            other = spot.along(axis, by)
            pltpu.make_async_remote_copy(
                src_ref=squares.at[axis, other], dst_ref=squares.at[axis, other], send_sem=ex_ssem.at[axis, by], recv_sem=ex_rsem.at[axis, other],
                device_id=spot.device(axis, by), device_id_type=MESH).wait_recv()
        part = squares[axis, 0]
        for i in range(1, side):
            part = part + squares[axis, i]
    total = jnp.sum(jnp.sum(part, 0, keepdims=True), 1, keepdims=True)
    factor = jnp.minimum(1.0, 0.5 * lax.rsqrt(total / count + 1e-30))

    for load in loads:
        load.wait()
    for kind in range(3):
        rows, columns = kinds[kind]

        def body(unit, carry):
            layer, unit = unit // (rows // UNIT), unit % (rows // UNIT)
            at = (layer, pl.ds(pl.multiple_of(unit * UNIT, UNIT), UNIT), slice(None))
            g = grad[kind][at].astype(F32) * factor
            m1 = 0.9 * m[kind][at] + 0.1 * g
            v1 = 0.95 * v[kind][at] + 0.05 * g * g
            wide = w[kind][at].astype(F32)
            m[kind][at], v[kind][at] = m1, v1
            fresh = (wide - 0.02 * (m1 * lax.rsqrt(v1 + 1e-8) + 0.1 * wide)).astype(BF16)
            terms[kind][(layer, *spot.at, *at[1:])] = fresh
            return carry

        lax.fori_loop(0, layers * (rows // UNIT), body, 0, unroll=2)

    class Gather:
        def __init__(self, half, kind):
            self.half, self.kind = half, kind
            self.rows, columns = kinds[kind]
            self.columns = pl.ds(half * (columns // 2), columns // 2)
            self.first, self.second = half, 1 - half
            self.base = 20 * (3 * half + kind)

        def place(self, by_first, by_second, some=slice(None)):
            a, b = spot.along(self.first, by_first), spot.along(self.second, by_second)
            x, y = (a, b) if self.half == 0 else (b, a)
            return terms[self.kind].at[some, x, y, :, self.columns]

        def go(self, index, way, axis, at):
            send(at, at, (ag_ssem, ag_rsem), self.base + index + way, spot.device(axis, 1 - 2 * way))

        def arrived(self, index, way, at):
            pltpu.make_async_remote_copy(
                src_ref=at, dst_ref=at, send_sem=ag_ssem.at[self.base + index + way], recv_sem=ag_rsem.at[self.base + index + way],
                device_id=spot.device(0, 1), device_id_type=MESH).wait_recv()

        def some(self, way):
            return pl.ds(way * (layers // 2), layers // 2)

        def start(self):
            for index, axis in ((0, self.first), (4, self.second)):
                for way in (0, 1):
                    self.go(index, way, axis, self.place(0, 0))

        def first_near(self, way):
            by = 2 * way - 1
            self.arrived(0, way, self.place(by, 0))
            self.go(2, way, self.first, self.place(by, 0, self.some(way)))
            for to in (0, 1):
                self.go(8 + 4 * way, to, self.second, self.place(by, 0))

        def first_far(self):
            for way in (0, 1):
                self.arrived(2, way, self.place(half_ring, 0, self.some(way)))
            for to in (0, 1):
                self.go(16, to, self.second, self.place(half_ring, 0))

        def second_near(self, which):
            by_first = (0, -1, 1, half_ring)[which]
            for way in (0, 1):
                by = 2 * way - 1
                self.arrived(4 + 4 * which, way, self.place(by_first, by))
                self.go(6 + 4 * which, way, self.second, self.place(by_first, by, self.some(way)))

        def second_far(self, which):
            by_first = (0, -1, 1, half_ring)[which]
            for way in (0, 1):
                self.arrived(6 + 4 * which, way, self.place(by_first, half_ring, self.some(way)))

    gathers = [Gather(half, kind) for kind in range(3) for half in (0, 1)]
    for gather in gathers:
        gather.start()
    for way in (0, 1):
        for gather in gathers:
            gather.first_near(way)
    for gather in gathers:
        gather.second_near(0)
    for gather in gathers:
        gather.first_far()
    for which in (1, 2, 3):
        for gather in gathers:
            gather.second_near(which)
    for which in range(4):
        for gather in gathers:
            gather.second_far(which)
    for copy in sent:
        copy.wait_send()


def solution(mesh):
    n = mesh.shape["dp"]
    side = math.isqrt(n)

    def update(products, dy, ws, ms, vs):
        layers, d, ff = ws[0].shape
        tokens = dy.shape[0]
        block = min(BLOCK, tokens // SEGMENTS)
        kinds = tuple((m.shape[1], m.shape[2]) for m in ms)
        count = float(sum(w.size for w in ws))
        vmem, dma = pltpu.VMEM, pltpu.SemaphoreType.DMA
        scratch = [vmem((2, d, tokens), BF16), vmem((2, max(tokens, 2 * d), ff // 2), BF16), vmem((ff, d), BF16)]
        scratch += [vmem((block, ff), BF16)] * 2 + [vmem((block, ff), F32)] * 2 + [vmem((block, d), BF16)] * 2 + [vmem((block, ff), BF16)] * 2
        scratch += [vmem((2, 2, side // 2, r, c // 2), BF16) for r, c in kinds]
        scratch += [vmem((2, 2, side, r, c // 2), BF16) for r, c in kinds]
        scratch += [vmem((layers, 2, r, c // 2), BF16) for r, c in kinds]
        scratch += [vmem((layers, 2, 2, r, c // 2), BF16) for r, c in kinds]
        scratch += [vmem((layers, 2, r, c // 2), F32) for r, c in kinds]
        for _ in range(2):
            scratch += [vmem((layers, r, c), BF16) for r, c in kinds]
        scratch += [vmem((2, side, 8, 128), F32)]
        sums, gathers = 8 * 2 * 3 * layers, 20 * 6
        scratch += [dma((3,)), dma((2,)), dma((5,)), dma((3, 4)), dma((9,)), dma((sums,)), dma((sums,)),
                    dma((2, side)), dma((2, side)), dma((gathers,)), dma((gathers,))]
        got = pl.pallas_call(
            functools.partial(kernel, side, kinds, count),
            out_shape=[vmem((layers, side, side, r, c), BF16) for r, c in kinds] + [vmem(m.shape, F32) for m in (*ms, *vs)]
            + [jax.ShapeDtypeStruct((tokens, ff), BF16)] * 2,
            in_specs=[ANY] * 20,
            out_specs=[HELD] * 9 + [ANY] * 2,
            scratch_shapes=scratch,
            compiler_params=pltpu.CompilerParams(collective_id=0, has_side_effects=True, vmem_limit_bytes=42 * 2**20),
        )(*products, dy, *ws, *ms, *vs)[:9]
        out = pl.pallas_call(
            write_kernel,
            out_shape=[jax.ShapeDtypeStruct(t.shape, t.dtype) for t in got],
            in_specs=[HELD] * 9,
            out_specs=[ANY] * 9,
            scratch_shapes=[dma((9, layers))],
            compiler_params=pltpu.CompilerParams(vmem_limit_bytes=4 * 2**20),
        )(*got)
        return [t.reshape(w.shape) for t, w in zip(out, (*ws, *ms, *vs))]

    def step(x, dy, *arrays):
        ws, ms, vs = (arrays[i : i + 3] for i in (0, 3, 6))
        return tuple(update(token_phase(x[0], dy[0], ws), dy[0], ws, ms, vs))

    data, whole, rows = P(("rep", "dp")), P(), P(None, "dp")
    return jax.shard_map(
        step, mesh=mesh,
        in_specs=(data, data, whole, whole, whole) + (rows,) * 6,
        out_specs=(P("rep"),) * 3 + (P("rep", "dp"),) * 6,
        check_vma=False,
    )
```
